128 devices in a mesh: row: 8 (over z, core), col: 16 (over y, x).
Axes of the slice: x: 4, y: 4, z: 4, core: 2. Of those that a mesh axis runs over, the one named last changes fastest.
Arguments:
- inverse_interior: float32 [8, 16, 1536, 1536], P('row', 'col'), may hold values from -0.15625 to 0.15625
- coupling: float32 [8, 16, 1536, 1024], P('row', 'col'), may hold values from -1 to 1
- interface_block: float32 [8, 16, 1024, 1024], P('row', 'col'), may hold values from -6 to 6
- iface_ids: int32 [8, 16, 4], P('row', 'col'), may hold values from 0 to 15, as said below
- row_place: int32 [16], replicated, may hold values from 0 to 15, as said below
- col_place: int32 [16], replicated, may hold values from 0 to 15, as said below
Outputs:
- assembled: float32 [16, 256, 16, 256], P('row', None, 'col')
The draws below stay inside these ranges and needn't reach their ends.
Inputs may be any that keep to these rules, and one draw needn't show every extreme that they name: `row_place`: A permutation of the tile ids. `col_place`: a permutation of the tile ids; two ids whose values of row_place differ mod 8 have values of col_place that differ mod 16. `iface_ids`: the 4 ids of one subdomain have pairwise different row_place mod 8, hence pairwise different col_place mod 16.
All inputs are finite; a program needn't handle non-finite values.
Results may differ from the reference program's by a relative error of at most 0.0001.
Values sent between devices are 32-bit elements; how exact they have to be, the bound alone decides.
No kernel may reach another device: no remote copies, remote signals or barrier semaphores. Data moves between devices by JAX's collectives and lax.ppermute only.
A program may use at most 192 MiB of HBM per device.

```python
import jax
import jax.numpy as jnp
from jax import lax

NG = 1024
TILE = 256
NI = 1536
OWN_R = 2
NB = 4
PROWS = 8
PCOLS = 16
NT = 16
OWN_C = 1


def layout(key):
    row_place = jax.random.permutation(jax.random.fold_in(key, 11), NT).astype(jnp.int32)
    position = jnp.arange(NT, dtype=jnp.int32)
    owner = row_place % PROWS
    scores = jax.random.permutation(jax.random.fold_in(key, 12), NT).astype(jnp.int32)
    same_owner = owner[:, None] == owner[None, :]
    ranking = jnp.sum(same_owner & (scores[None, :] < scores[:, None]), axis=1).astype(jnp.int32)
    spread = PCOLS // PROWS
    col_owner = owner * spread + ranking % spread
    col_place = (ranking // spread * PCOLS + col_owner).astype(jnp.int32)
    inverse = jnp.zeros((NT,), jnp.int32).at[row_place].set(position)
    devices = PROWS * PCOLS
    weights = jax.random.randint(jax.random.fold_in(key, 13), (devices, PROWS), 0, 1 << 20).astype(jnp.int32)
    weights = weights * PROWS + jnp.arange(PROWS, dtype=jnp.int32)[None, :]
    owners = jnp.argsort(weights, axis=1)[:, :NB].astype(jnp.int32)
    slot_draw = jax.random.randint(jax.random.fold_in(key, 14), (devices, NB), 0, OWN_R).astype(jnp.int32)
    global_ids = inverse[slot_draw * PROWS + owners].astype(jnp.int32)
    return (row_place, col_place, global_ids.reshape(PROWS, PCOLS, NB))


def draw_row_place(key, part):
    return layout(key)[0]


def draw_col_place(key, part):
    return layout(key)[1]


def draw_iface_ids(key, part):
    return layout(key)[2]


def level_of(stream_key, shape, shards, smallest, top_value):
    factor_of, own = 1.0, jax.random.fold_in(stream_key, 6)
    for dim, parts in shards:
        heights = jnp.exp(jax.random.uniform(jax.random.fold_in(own, dim), (parts,), jnp.float32, smallest / len(shards), top_value / len(shards)))
        factor_of = factor_of * jnp.repeat(heights, shape[dim] // parts).reshape([-1 if axis == dim else 1 for axis in range(len(shape))])
    return factor_of


def noise(key, extent, width, reach, split=(), kind=jnp.bfloat16):
    factor_of = level_of(key, extent, split, -0.22, 0.18) if split else 1.0
    values = jax.random.normal(key, extent, jnp.float32) * width * factor_of
    return jnp.minimum(jnp.maximum(values, -reach), reach).astype(kind)


def setup_inputs(seed: int = 0) -> dict:
    key_list = jax.random.split(jax.random.key(seed), 7)
    return {
        "inverse_interior": noise(key_list[0], (PROWS, PCOLS, NI, NI), NI ** -0.5, 0.15625, ((0, 8), (1, 16)), jnp.float32),
        "coupling": noise(key_list[1], (PROWS, PCOLS, NI, NG), 0.16, 1.0, ((0, 8), (1, 16)), jnp.float32),
        "interface_block": noise(key_list[2], (PROWS, PCOLS, NG, NG), 1.0, 6.0, ((0, 8), (1, 16)), jnp.float32),
        "iface_ids": draw_iface_ids(jax.random.fold_in(key_list[6], 71), 0),
        "row_place": draw_row_place(jax.random.fold_in(key_list[6], 71), 0),
        "col_place": draw_col_place(jax.random.fold_in(key_list[6], 71), 0),
    }


def reference(inverse_interior, coupling, interface_block, iface_ids, row_place, col_place):
    highest = lax.Precision.HIGHEST
    out_rows = ((row_place % PROWS) * OWN_R + row_place // PROWS).astype(jnp.int32)
    out_cols = ((col_place % PCOLS) * OWN_C + col_place // PCOLS).astype(jnp.int32)
    tile_count = NG // TILE
    devices = PROWS * PCOLS

    def absorb(accum, items):
        inverse, couple, block, global_ids = items
        solved = jnp.dot(inverse, couple, precision=highest, preferred_element_type=jnp.float32)
        product = lax.dot_general(couple, solved, (((0,), (0,)), ((), ())), precision=highest, preferred_element_type=jnp.float32)
        schur_block = block - product
        tile_grid = schur_block.reshape(tile_count, TILE, tile_count, TILE).transpose(0, 2, 1, 3)
        row_index = out_rows[global_ids]
        col_index = out_cols[global_ids]
        accum = accum.at[row_index[:, None], :, col_index[None, :], :].add(tile_grid)
        return accum, None

    items = (inverse_interior.reshape(devices, NI, NI), coupling.reshape(devices, NI, NG), interface_block.reshape(devices, NG, NG), iface_ids.reshape(devices, NB))
    initial = jnp.zeros((NT, TILE, NT, TILE), jnp.float32)
    accum, ignored = lax.scan(absorb, initial, items)
    return accum
```

```python
import jax
import jax.numpy as jnp
from jax import lax
from jax.experimental import pallas as pl
from jax.experimental.pallas import tpu as pltpu
from jax.sharding import PartitionSpec as P

TILE = 256
AXES = ("row", "col")
STEP = 16


def combine_kernel(ids_ref, row_ref, col_ref, *refs):
    parts, out_ref = refs[:-1], refs[-1]
    step = pl.program_id(0)

    @pl.when(step == 0)
    def _():
        out_ref[...] = jnp.zeros(out_ref.shape, jnp.float32)

    def absorb(k, carry):
        source = step * STEP + k
        row_base, col_base = [], []
        for a in range(4):
            g = ids_ref[source, a]
            rp = row_ref[g]
            row_base.append((rp & 7) * 32 + (rp >> 3))
            col_base.append(col_ref[g] * 2)
        places, values = [], []
        count = 0
        for part in parts:
            for t in range(part.shape[1]):
                place = row_base[count // 4] + col_base[count % 4]
                places.append(place)
                values.append(out_ref[place] + part[k, t])
                count += 1
        for place, value in zip(places, values):
            out_ref[place] = value
        return carry

    lax.fori_loop(0, STEP, absorb, 0, unroll=2)


def combine(ids, row_place, col_place, parts):
    smem = pl.BlockSpec(memory_space=pltpu.SMEM)
    return pl.pallas_call(
        combine_kernel,
        grid=(ids.shape[0] // STEP,),
        in_specs=[smem, smem, smem]
        + [pl.BlockSpec((STEP,) + p.shape[1:], lambda s: (s, 0, 0, 0)) for p in parts],
        out_specs=pl.BlockSpec((256, 4, 128), lambda s: (0, 0, 0)),
        out_shape=jax.ShapeDtypeStruct((256, 4, 128), jnp.float32),
        name="combine",
    )(ids, row_place, col_place, *parts)


def on_device(inverse_interior, coupling, interface_block, iface_ids, row_place, col_place):
    inverse = inverse_interior[0, 0]
    couple = coupling[0, 0]
    block = interface_block[0, 0]
    ids = lax.all_to_all(
        jnp.broadcast_to(iface_ids[0, 0][None, :], (128, 4)), AXES, 0, 0, tiled=True
    )
    arrived = []
    for first, last in ((0, 2), (2, 4)):
        rows = slice(first * TILE, last * TILE)
        left = lax.dot_general(
            couple[:, rows],
            inverse,
            (((0,), (0,)), ((), ())),
            precision=lax.Precision.HIGH,
            preferred_element_type=jnp.float32,
        )
        schur = block[rows] - jnp.dot(
            left, couple, precision=lax.Precision.HIGH, preferred_element_type=jnp.float32
        )
        pieces = schur.reshape(last - first, 32, 2, 4, 4, 2, 128)
        pieces = pieces.transpose(1, 5, 2, 0, 4, 3, 6).reshape(128, (last - first) * 4, 4, 128)
        arrived.append(lax.all_to_all(pieces, AXES, 0, 0, tiled=True))
    total = combine(ids, row_place, col_place, arrived)
    owned = lax.all_to_all(total.reshape(128, 2, 4, 128), AXES, 0, 0, tiled=True)
    owned = owned.reshape(32, 2, 2, 2, 4, 128).transpose(3, 0, 2, 4, 1, 5)
    return owned.reshape(2, TILE, 1, TILE)


def solution(mesh):
    return jax.shard_map(
        on_device,
        mesh=mesh,
        in_specs=(
            P("row", "col", None, None),
            P("row", "col", None, None),
            P("row", "col", None, None),
            P("row", "col", None),
            P(),
            P(),
        ),
        out_specs=P("row", None, "col", None),
        check_vma=False,
    )
```

```python
import functools

import jax
import jax.numpy as jnp
from jax import lax
from jax.experimental import pallas as pl
from jax.experimental.pallas import tpu as pltpu
from jax.sharding import PartitionSpec as P

TILE = 256
AXES = ("row", "col")
SOLVE_ROWS = 512
SCHUR_ROWS = 512
PACK = 65


def split(x):
    high = x.astype(jnp.bfloat16)
    return high, (x - high.astype(jnp.float32)).astype(jnp.bfloat16)


def dot3(xh, xl, yh, yl, dims):
    def dot(x, y):
        return lax.dot_general(x, y, (dims, ((), ())), preferred_element_type=jnp.float32)

    return dot(xh, yh) + (dot(xh, yl) + dot(xl, yh))


def schur_kernel(
    ids_ref, row_ref, col_ref, inverse_ref, couple_ref, block_ref, out_ref, ch_ref, cl_ref, uh_ref, ul_ref, *, solves, schurs
):
    step = pl.program_id(0)

    @pl.when(step == 0)
    def _():
        ch_ref[...], cl_ref[...] = split(couple_ref[...])
        lane = lax.broadcasted_iota(jnp.int32, (128, 128), 1)
        marks = jnp.zeros((128, 128), jnp.int32)
        for t in range(16):
            row = row_ref[ids_ref[t // 4]]
            col = col_ref[ids_ref[t % 4]]
            place = ((row & 7) * 16 + col) * 2 + (row >> 3)
            marks = jnp.where(lane == t, place, marks)
        out_ref[pl.ds(64, 128, stride=PACK), :] = marks.astype(jnp.float32)

    @pl.when(step < solves)
    def _():
        high, low = split(inverse_ref[...])
        solved = dot3(high, low, ch_ref[...], cl_ref[...], ((1,), (0,)))
        rows = pl.ds(step * SOLVE_ROWS, SOLVE_ROWS)
        uh_ref[rows, :], ul_ref[rows, :] = split(solved)

    for part in range(schurs):

        @pl.when(step == solves + part)
        def _():
            cols = slice(part * SCHUR_ROWS, (part + 1) * SCHUR_ROWS)
            product = dot3(ch_ref[:, cols], cl_ref[:, cols], uh_ref[...], ul_ref[...], ((0,), (0,)))
            schur = block_ref[...] - product
            for t in range(SCHUR_ROWS // TILE * 4):
                a, b = divmod(t, 4)
                for lane in range(2):
                    left = b * TILE + lane * 128
                    for group in range(32):
                        for half in range(2):
                            top = a * TILE + group * 8 + half * 4
                            start = (group * 4 + lane * 2 + half) * PACK + (part * SCHUR_ROWS // TILE * 4 + t) * 4
                            out_ref[start : start + 4, :] = schur[top : top + 4, left : left + 128]


def schur_tiles(ids, row_place, col_place, inverse, couple, block):
    inner, outer = couple.shape
    solves, schurs = inner // SOLVE_ROWS, outer // SCHUR_ROWS
    smem = pl.BlockSpec(memory_space=pltpu.SMEM)
    return pl.pallas_call(
        functools.partial(schur_kernel, solves=solves, schurs=schurs),
        grid=(solves + schurs,),
        in_specs=[
            smem,
            smem,
            smem,
            pl.BlockSpec((SOLVE_ROWS, inner), lambda s: (jnp.minimum(s, solves - 1), 0)),
            pl.BlockSpec((inner, outer), lambda s: (0, 0)),
            pl.BlockSpec((SCHUR_ROWS, outer), lambda s: (jnp.clip(s - solves, 0, schurs - 1), 0)),
        ],
        out_specs=pl.BlockSpec(memory_space=pltpu.VMEM),
        out_shape=pltpu.VMEM((128 * PACK, 128), jnp.float32),
        scratch_shapes=[pltpu.VMEM((inner, outer), jnp.bfloat16)] * 4,
        compiler_params=pltpu.CompilerParams(vmem_limit_bytes=54 * 1024 * 1024),
        cost_estimate=pl.CostEstimate(flops=24 * 10**9, bytes_accessed=25 * 10**6, transcendentals=0),
        name="schur",
    )(ids, row_place, col_place, inverse, couple, block)


def combine_kernel(part_ref, out_ref, place_ref, high_ref, low_ref):
    marks = part_ref[pl.ds(64, 128, stride=PACK), :]
    spots = lax.broadcasted_iota(jnp.int32, (128, 256), 1).astype(jnp.float32)
    for t in range(16):
        rows = slice(t * 128, (t + 1) * 128)
        hit = jnp.broadcast_to(marks[:, t : t + 1], (128, 256)) == spots
        place_ref[rows, :] = jnp.where(hit, 1.0, 0.0).astype(jnp.bfloat16)
        for r in range(4):
            lanes = slice(r * 128, (r + 1) * 128)
            values = part_ref[pl.ds(t * 4 + r, 128, stride=PACK), :]
            high_ref[rows, lanes], low_ref[rows, lanes] = split(values)

    def total(values):
        return lax.dot_general(
            place_ref[...], values, (((0,), (0,)), ((), ())), preferred_element_type=jnp.float32
        )

    sums = total(high_ref[...]) + total(low_ref[...])
    for r in range(4):
        out_ref[pl.ds(r, 256, stride=4), :] = sums[:, r * 128 : (r + 1) * 128]


def combine(parts):
    parts = pltpu.with_memory_space_constraint(parts, pltpu.VMEM)
    return pl.pallas_call(
        combine_kernel,
        in_specs=[pl.BlockSpec(memory_space=pltpu.VMEM)],
        out_specs=pl.BlockSpec(memory_space=pltpu.VMEM),
        out_shape=pltpu.VMEM((1024, 128), jnp.float32),
        scratch_shapes=[
            pltpu.VMEM((2048, 256), jnp.bfloat16),
            pltpu.VMEM((2048, 512), jnp.bfloat16),
            pltpu.VMEM((2048, 512), jnp.bfloat16),
        ],
        compiler_params=pltpu.CompilerParams(vmem_limit_bytes=24 * 1024 * 1024),
        name="combine",
    )(parts)


def on_device(inverse_interior, coupling, interface_block, iface_ids, row_place, col_place):
    pieces = schur_tiles(
        iface_ids[0, 0], row_place, col_place, inverse_interior[0, 0], coupling[0, 0], interface_block[0, 0]
    )
    arrived = lax.all_to_all(pieces.reshape(128, PACK, 1, 128), AXES, 0, 0, tiled=True)
    total = combine(arrived.reshape(128 * PACK, 128))
    owned = lax.all_to_all(total.reshape(128, 8, 128), AXES, 0, 0, tiled=True)
    owned = owned.reshape(32, 2, 2, 2, 4, 128).transpose(3, 0, 2, 4, 1, 5)
    return owned.reshape(2, TILE, 1, TILE)


def solution(mesh):
    return jax.shard_map(
        on_device,
        mesh=mesh,
        in_specs=(
            P("row", "col", None, None),
            P("row", "col", None, None),
            P("row", "col", None, None),
            P("row", "col", None),
            P(),
            P(),
        ),
        out_specs=P("row", None, "col", None),
        check_vma=False,
    )
```

```python
import functools

import jax
import jax.numpy as jnp
from jax import lax
from jax.experimental import pallas as pl
from jax.experimental.pallas import tpu as pltpu
from jax.sharding import PartitionSpec as P

TILE = 256
AXES = ("row", "col")
DEPTH = 256
SCHUR_ROWS = 512
PACK = 65


def pack_row(a, u, b, h):
    return a * 16 + u * 8 + b * 2 + h


def split(x):
    high = x.astype(jnp.bfloat16)
    return high, (x - high.astype(jnp.float32)).astype(jnp.bfloat16)


def dot(x, y, dims):
    return lax.dot_general(x, y, (dims, ((), ())), preferred_element_type=jnp.float32)


def schur_kernel(
    ids_ref,
    row_ref,
    col_ref,
    inverse_ref,
    couple_ref,
    block_hbm,
    out_ref,
    left_ref,
    right_ref,
    ch_ref,
    cl_ref,
    sum_ref,
    uh_ref,
    ul_ref,
    block_ref,
    block_sem,
    *,
    depths,
    schurs,
):
    step = pl.program_id(0)
    fetch = pltpu.make_async_copy(block_hbm, block_ref, block_sem)

    @pl.when(step == 0)
    def _():
        lane = lax.broadcasted_iota(jnp.int32, (128, 128), 1)
        marks = jnp.zeros((128, 128), jnp.int32)
        for t in range(16):
            row = row_ref[ids_ref[t // 4]]
            col = col_ref[ids_ref[t % 4]]
            place = ((row & 7) * 16 + col) * 2 + (row >> 3)
            marks = jnp.where(lane == t, place, marks)
        out_ref[pl.ds(64, 128, stride=PACK), :] = marks.astype(jnp.float32)

    def partial():
        high, low = split(inverse_ref[...])
        left_ref[:, :DEPTH] = high
        left_ref[:, DEPTH : 2 * DEPTH] = low
        left_ref[:, 2 * DEPTH :] = high
        high, low = split(couple_ref[...])
        right_ref[:DEPTH, :] = high
        right_ref[DEPTH : 2 * DEPTH, :] = high
        right_ref[2 * DEPTH :, :] = low
        rows = pl.ds(step * DEPTH, DEPTH)
        ch_ref[rows, :] = high
        cl_ref[rows, :] = low
        return dot(left_ref[...], right_ref[...], ((1,), (0,)))

    @pl.when(step == 0)
    def _():
        sum_ref[...] = partial()

    @pl.when((step > 0) & (step < depths - 1))
    def _():
        sum_ref[...] += partial()

    @pl.when(step == 1)
    def _():
        fetch.start()

    @pl.when(step == depths - 1)
    def _():
        uh_ref[...], ul_ref[...] = split(sum_ref[...] + partial())
        fetch.wait()

    for part in range(schurs):

        @pl.when(step == depths + part)
        def _():
            cols = slice(part * SCHUR_ROWS, (part + 1) * SCHUR_ROWS)
            ch, cl, uh, ul = ch_ref[:, cols], cl_ref[:, cols], uh_ref[...], ul_ref[...]
            across = ((0,), (0,))
            schur = block_ref[cols, :] - (dot(ch, uh, across) + (dot(ch, ul, across) + dot(cl, uh, across)))
            for n in range(SCHUR_ROWS // 128):
                a, u = divmod(part * SCHUR_ROWS // 128 + n, 2)
                for b in range(4):
                    for h in range(2):
                        left = b * TILE + h * 128
                        out_ref[pl.ds(pack_row(a, u, b, h), 128, stride=PACK), :] = schur[
                            n * 128 : (n + 1) * 128, left : left + 128
                        ]


def schur_tiles(ids, row_place, col_place, inverse, couple, block):
    inner, outer = couple.shape
    depths, schurs = inner // DEPTH, outer // SCHUR_ROWS
    smem = pl.BlockSpec(memory_space=pltpu.SMEM)
    return pl.pallas_call(
        functools.partial(schur_kernel, depths=depths, schurs=schurs),
        grid=(depths + schurs,),
        in_specs=[
            smem,
            smem,
            smem,
            pl.BlockSpec((inner, DEPTH), lambda s: (0, jnp.minimum(s, depths - 1))),
            pl.BlockSpec((DEPTH, outer), lambda s: (jnp.minimum(s, depths - 1), 0)),
            pl.BlockSpec(memory_space=pltpu.HBM),
        ],
        out_specs=pl.BlockSpec(memory_space=pltpu.VMEM),
        out_shape=pltpu.VMEM((128 * PACK, 128), jnp.float32),
        scratch_shapes=[
            pltpu.VMEM((inner, 3 * DEPTH), jnp.bfloat16),
            pltpu.VMEM((3 * DEPTH, outer), jnp.bfloat16),
            pltpu.VMEM((inner, outer), jnp.bfloat16),
            pltpu.VMEM((inner, outer), jnp.bfloat16),
            pltpu.VMEM((inner, outer), jnp.float32),
            pltpu.VMEM((inner, outer), jnp.bfloat16),
            pltpu.VMEM((inner, outer), jnp.bfloat16),
            pltpu.VMEM((outer, outer), jnp.float32),
            pltpu.SemaphoreType.DMA,
        ],
        compiler_params=pltpu.CompilerParams(vmem_limit_bytes=56 * 1024 * 1024),
        cost_estimate=pl.CostEstimate(flops=24 * 10**9, bytes_accessed=25 * 10**6, transcendentals=0),
        name="schur",
    )(ids, row_place, col_place, inverse, couple, block)


def combine_kernel(part_ref, out_ref, place_ref, high_ref, low_ref):
    marks = part_ref[pl.ds(64, 128, stride=PACK), :]
    spots = lax.broadcasted_iota(jnp.int32, (128, 256), 1).astype(jnp.float32)
    for t in range(16):
        rows = slice(t * 128, (t + 1) * 128)
        hit = jnp.broadcast_to(marks[:, t : t + 1], (128, 256)) == spots
        place_ref[rows, :] = jnp.where(hit, 1.0, 0.0).astype(jnp.bfloat16)
        for r in range(4):
            lanes = slice(r * 128, (r + 1) * 128)
            row = pack_row(t // 4, r // 2, t % 4, r % 2)
            values = part_ref[pl.ds(row, 128, stride=PACK), :]
            high_ref[rows, lanes], low_ref[rows, lanes] = split(values)

    def total(values):
        return lax.dot_general(
            place_ref[...], values, (((0,), (0,)), ((), ())), preferred_element_type=jnp.float32
        )

    sums = total(high_ref[...]) + total(low_ref[...])
    for r in range(4):
        out_ref[pl.ds(r, 256, stride=4), :] = sums[:, r * 128 : (r + 1) * 128]


def combine(parts):
    parts = pltpu.with_memory_space_constraint(parts, pltpu.VMEM)
    return pl.pallas_call(
        combine_kernel,
        in_specs=[pl.BlockSpec(memory_space=pltpu.VMEM)],
        out_specs=pl.BlockSpec(memory_space=pltpu.VMEM),
        out_shape=pltpu.VMEM((1024, 128), jnp.float32),
        scratch_shapes=[
            pltpu.VMEM((2048, 256), jnp.bfloat16),
            pltpu.VMEM((2048, 512), jnp.bfloat16),
            pltpu.VMEM((2048, 512), jnp.bfloat16),
        ],
        compiler_params=pltpu.CompilerParams(vmem_limit_bytes=24 * 1024 * 1024),
        name="combine",
    )(parts)


def on_device(inverse_interior, coupling, interface_block, iface_ids, row_place, col_place):
    pieces = schur_tiles(
        iface_ids[0, 0], row_place, col_place, inverse_interior[0, 0], coupling[0, 0], interface_block[0, 0]
    )
    arrived = lax.all_to_all(pieces.reshape(128, PACK, 1, 128), AXES, 0, 0, tiled=True)
    total = combine(arrived.reshape(128 * PACK, 128))
    owned = lax.all_to_all(total.reshape(128, 8, 128), AXES, 0, 0, tiled=True)
    owned = owned.reshape(128, 2, 2, 2, 128).transpose(1, 2, 0, 3, 4)
    return owned.reshape(2, TILE, 1, TILE)


def solution(mesh):
    return jax.shard_map(
        on_device,
        mesh=mesh,
        in_specs=(
            P("row", "col", None, None),
            P("row", "col", None, None),
            P("row", "col", None, None),
            P("row", "col", None),
            P(),
            P(),
        ),
        out_specs=P("row", None, "col", None),
        check_vma=False,
    )
```

```python
import functools

import jax
import jax.numpy as jnp
from jax import lax
from jax.experimental import pallas as pl
from jax.experimental.pallas import tpu as pltpu
from jax.sharding import PartitionSpec as P

TILE = 256
AXES = ("row", "col")
DEPTH = 256
SCHUR_ROWS = 512
PACK = 65


def pack_row(a, u, b, h):
    return a * 16 + u * 8 + b * 2 + h


def split(x):
    high = x.astype(jnp.bfloat16)
    return high, (x - high.astype(jnp.float32)).astype(jnp.bfloat16)


def dot(x, y, dims):
    return lax.dot_general(x, y, (dims, ((), ())), preferred_element_type=jnp.float32)


def schur_kernel(
    ids_ref,
    row_ref,
    col_ref,
    inverse_ref,
    couple_ref,
    block_hbm,
    out_ref,
    left_ref,
    right_ref,
    ch_ref,
    cl_ref,
    sum_ref,
    uh_ref,
    ul_ref,
    block_ref,
    block_sem,
    *,
    depths,
    schurs,
):
    step = pl.program_id(0)
    fetch = pltpu.make_async_copy(block_hbm, block_ref, block_sem)

    @pl.when(step == 0)
    def _():
        lane = lax.broadcasted_iota(jnp.int32, (128, 128), 1)
        marks = jnp.zeros((128, 128), jnp.int32)
        for t in range(16):
            row = row_ref[ids_ref[t // 4]]
            col = col_ref[ids_ref[t % 4]]
            place = ((row & 7) * 16 + col) * 2 + (row >> 3)
            marks = jnp.where(lane == t, place, marks)
        out_ref[pl.ds(64, 128, stride=PACK), :] = marks.astype(jnp.float32)

    def partial():
        high, low = split(inverse_ref[...])
        left_ref[:, :DEPTH] = high
        left_ref[:, DEPTH : 2 * DEPTH] = low
        left_ref[:, 2 * DEPTH :] = high
        high, low = split(couple_ref[...])
        right_ref[:DEPTH, :] = high
        right_ref[DEPTH : 2 * DEPTH, :] = high
        right_ref[2 * DEPTH :, :] = low
        rows = pl.ds(step * DEPTH, DEPTH)
        ch_ref[rows, :] = high
        cl_ref[rows, :] = low
        return dot(left_ref[...], right_ref[...], ((1,), (0,)))

    @pl.when(step == 0)
    def _():
        sum_ref[...] = partial()

    @pl.when((step > 0) & (step < depths - 1))
    def _():
        sum_ref[...] += partial()

    @pl.when(step == 1)
    def _():
        fetch.start()

    @pl.when(step == depths - 1)
    def _():
        uh_ref[...], ul_ref[...] = split(sum_ref[...] + partial())
        fetch.wait()

    for part in range(schurs):

        @pl.when(step == depths + part)
        def _():
            cols = slice(part * SCHUR_ROWS, (part + 1) * SCHUR_ROWS)
            ch, cl, uh, ul = ch_ref[:, cols], cl_ref[:, cols], uh_ref[...], ul_ref[...]
            across = ((0,), (0,))
            schur = block_ref[cols, :] - (dot(ch, uh, across) + (dot(ch, ul, across) + dot(cl, uh, across)))
            for n in range(SCHUR_ROWS // 128):
                a, u = divmod(part * SCHUR_ROWS // 128 + n, 2)
                for b in range(4):
                    for h in range(2):
                        left = b * TILE + h * 128
                        out_ref[pl.ds(pack_row(a, u, b, h), 128, stride=PACK), :] = schur[
                            n * 128 : (n + 1) * 128, left : left + 128
                        ]


def schur_tiles(ids, row_place, col_place, inverse, couple, block):
    inner, outer = couple.shape
    depths, schurs = inner // DEPTH, outer // SCHUR_ROWS
    smem = pl.BlockSpec(memory_space=pltpu.SMEM)
    return pl.pallas_call(
        functools.partial(schur_kernel, depths=depths, schurs=schurs),
        grid=(depths + schurs,),
        in_specs=[
            smem,
            smem,
            smem,
            pl.BlockSpec((inner, DEPTH), lambda s: (0, jnp.minimum(s, depths - 1))),
            pl.BlockSpec((DEPTH, outer), lambda s: (jnp.minimum(s, depths - 1), 0)),
            pl.BlockSpec(memory_space=pltpu.HBM),
        ],
        out_specs=pl.BlockSpec(memory_space=pltpu.VMEM),
        out_shape=pltpu.VMEM((128 * PACK, 128), jnp.float32),
        scratch_shapes=[
            pltpu.VMEM((inner, 3 * DEPTH), jnp.bfloat16),
            pltpu.VMEM((3 * DEPTH, outer), jnp.bfloat16),
            pltpu.VMEM((inner, outer), jnp.bfloat16),
            pltpu.VMEM((inner, outer), jnp.bfloat16),
            pltpu.VMEM((inner, outer), jnp.float32),
            pltpu.VMEM((inner, outer), jnp.bfloat16),
            pltpu.VMEM((inner, outer), jnp.bfloat16),
            pltpu.VMEM((outer, outer), jnp.float32),
            pltpu.SemaphoreType.DMA,
        ],
        compiler_params=pltpu.CompilerParams(vmem_limit_bytes=56 * 1024 * 1024),
        cost_estimate=pl.CostEstimate(flops=24 * 10**9, bytes_accessed=25 * 10**6, transcendentals=0),
        name="schur",
    )(ids, row_place, col_place, inverse, couple, block)


def combine_kernel(part_ref, out_ref):
    marks = part_ref[pl.ds(64, 128, stride=PACK), :].T
    spots = lax.broadcasted_iota(jnp.int32, (256, 128), 0).astype(jnp.float32)
    sums = jnp.zeros((256, 512), jnp.float32)
    for a in range(4):
        places, highs, lows = [], [], []
        for b in range(4):
            t = a * 4 + b
            hit = jnp.broadcast_to(marks[t : t + 1, :], (256, 128)) == spots
            places.append(jnp.where(hit, 1.0, 0.0).astype(jnp.bfloat16))
            values = jnp.concatenate(
                [part_ref[pl.ds(pack_row(a, r // 2, b, r % 2), 128, stride=PACK), :] for r in range(4)], axis=1
            )
            high, low = split(values)
            highs.append(high)
            lows.append(low)
        place = jnp.concatenate(places + places, axis=1)
        sums = sums + jnp.dot(place, jnp.concatenate(highs + lows, axis=0), preferred_element_type=jnp.float32)
    for r in range(4):
        out_ref[pl.ds(r, 256, stride=4), :] = sums[:, r * 128 : (r + 1) * 128]


def combine(parts):
    parts = pltpu.with_memory_space_constraint(parts, pltpu.VMEM)
    return pl.pallas_call(
        combine_kernel,
        in_specs=[pl.BlockSpec(memory_space=pltpu.VMEM)],
        out_specs=pl.BlockSpec(memory_space=pltpu.VMEM),
        out_shape=pltpu.VMEM((1024, 128), jnp.float32),
        compiler_params=pltpu.CompilerParams(vmem_limit_bytes=24 * 1024 * 1024),
        name="combine",
    )(parts)


def on_device(inverse_interior, coupling, interface_block, iface_ids, row_place, col_place):
    pieces = schur_tiles(
        iface_ids[0, 0], row_place, col_place, inverse_interior[0, 0], coupling[0, 0], interface_block[0, 0]
    )
    arrived = lax.all_to_all(pieces.reshape(128, PACK, 1, 128), AXES, 0, 0, tiled=True)
    total = combine(arrived.reshape(128 * PACK, 128))
    owned = lax.all_to_all(total.reshape(128, 8, 128), AXES, 0, 0, tiled=True)
    owned = owned.reshape(128, 2, 2, 2, 128).transpose(1, 2, 0, 3, 4)
    return owned.reshape(2, TILE, 1, TILE)


def solution(mesh):
    return jax.shard_map(
        on_device,
        mesh=mesh,
        in_specs=(
            P("row", "col", None, None),
            P("row", "col", None, None),
            P("row", "col", None, None),
            P("row", "col", None),
            P(),
            P(),
        ),
        out_specs=P("row", None, "col", None),
        check_vma=False,
    )
```

```python
import functools

import jax
import jax.numpy as jnp
from jax import lax
from jax.experimental import pallas as pl
from jax.experimental.pallas import tpu as pltpu
from jax.sharding import PartitionSpec as P

TILE = 256
AXES = ("row", "col")
CUTS = (0, 256, 768, 1536)
SCHUR_ROWS = 1024
PACK = 65


def pack_row(a, u, b, h):
    return a * 16 + u * 8 + b * 2 + h


def split(x):
    high = x.astype(jnp.bfloat16)
    return high, (x - high.astype(jnp.float32)).astype(jnp.bfloat16)


def dot(x, y, dims):
    return lax.dot_general(x, y, (dims, ((), ())), preferred_element_type=jnp.float32)


def schur_kernel(
    ids_ref,
    row_ref,
    col_ref,
    inverse_hbm,
    couple_hbm,
    block_hbm,
    out_ref,
    inverse_ref,
    couple_ref,
    block_ref,
    ch_ref,
    cl_ref,
    sum_ref,
    uh_ref,
    ul_ref,
    sems,
    block_sem,
):
    outer = couple_ref.shape[1]
    schurs = outer // SCHUR_ROWS
    bounds = list(zip(CUTS[:-1], CUTS[1:]))

    def fetches(n):
        depth = slice(*bounds[n])
        return [
            pltpu.make_async_copy(couple_hbm.at[depth], couple_ref.at[depth], sems.at[n, 0]),
            pltpu.make_async_copy(inverse_hbm.at[:, depth], inverse_ref.at[:, depth], sems.at[n, 1]),
        ]

    def start(n):
        for fetch in fetches(n):
            fetch.start()

    step = pl.program_id(0)
    fetch_block = pltpu.make_async_copy(block_hbm, block_ref, block_sem)

    @pl.when(step == 0)
    def _():
        start(0)
        start(1)
        lane = lax.broadcasted_iota(jnp.int32, (128, 128), 1)
        marks = jnp.zeros((128, 128), jnp.int32)
        for t in range(16):
            row = row_ref[ids_ref[t // 4]]
            col = col_ref[ids_ref[t % 4]]
            place = ((row & 7) * 16 + col) * 2 + (row >> 3)
            marks = jnp.where(lane == t, place, marks)
        out_ref[pl.ds(64, 128, stride=PACK), :] = marks.astype(jnp.float32)

    def deepen(n):
        for fetch in fetches(n):
            fetch.wait()
        if n + 2 < len(bounds):
            start(n + 2)
        elif n + 2 == len(bounds):
            fetch_block.start()
        depth = slice(*bounds[n])
        ah, al = split(inverse_ref[:, depth])
        ch, cl = split(couple_ref[depth, :])
        ch_ref[depth, :] = ch
        cl_ref[depth, :] = cl
        across = ((1,), (0,))
        product = dot(ah, ch, across) + (dot(ah, cl, across) + dot(al, ch, across))
        if n == 0:
            sum_ref[...] = product
        elif n < len(bounds) - 1:
            sum_ref[...] += product
        else:
            uh_ref[...], ul_ref[...] = split(sum_ref[...] + product)
            fetch_block.wait()

    def finish(part):
        cols = slice(part * SCHUR_ROWS, (part + 1) * SCHUR_ROWS)
        ch, cl, uh, ul = ch_ref[:, cols], cl_ref[:, cols], uh_ref[...], ul_ref[...]
        across = ((0,), (0,))
        schur = block_ref[cols, :] - (dot(ch, uh, across) + (dot(ch, ul, across) + dot(cl, uh, across)))
        for n in range(SCHUR_ROWS // 128):
            a, u = divmod(part * SCHUR_ROWS // 128 + n, 2)
            for b in range(4):
                for h in range(2):
                    left = b * TILE + h * 128
                    out_ref[pl.ds(pack_row(a, u, b, h), 128, stride=PACK), :] = schur[
                        n * 128 : (n + 1) * 128, left : left + 128
                    ]

    for n in range(len(bounds)):
        pl.when(step == n)(functools.partial(deepen, n))
    for part in range(schurs):
        pl.when(step == len(bounds) + part)(functools.partial(finish, part))


def schur_tiles(ids, row_place, col_place, inverse, couple, block):
    inner, outer = couple.shape
    smem = pl.BlockSpec(memory_space=pltpu.SMEM)
    hbm = pl.BlockSpec(memory_space=pltpu.HBM)
    return pl.pallas_call(
        schur_kernel,
        grid=(len(CUTS) - 1 + outer // SCHUR_ROWS,),
        in_specs=[smem, smem, smem, hbm, hbm, hbm],
        out_specs=pl.BlockSpec(memory_space=pltpu.VMEM),
        out_shape=pltpu.VMEM((128 * PACK, 128), jnp.float32),
        scratch_shapes=[
            pltpu.VMEM((inner, inner), jnp.float32),
            pltpu.VMEM((inner, outer), jnp.float32),
            pltpu.VMEM((outer, outer), jnp.float32),
            pltpu.VMEM((inner, outer), jnp.bfloat16),
            pltpu.VMEM((inner, outer), jnp.bfloat16),
            pltpu.VMEM((inner, outer), jnp.float32),
            pltpu.VMEM((inner, outer), jnp.bfloat16),
            pltpu.VMEM((inner, outer), jnp.bfloat16),
            pltpu.SemaphoreType.DMA((len(CUTS) - 1, 2)),
            pltpu.SemaphoreType.DMA,
        ],
        compiler_params=pltpu.CompilerParams(vmem_limit_bytes=57 * 1024 * 1024),
        cost_estimate=pl.CostEstimate(flops=24 * 10**9, bytes_accessed=25 * 10**6, transcendentals=0),
        name="schur",
    )(ids, row_place, col_place, inverse, couple, block)


def combine_kernel(part_ref, out_ref):
    marks = part_ref[pl.ds(64, 128, stride=PACK), :].T
    spots = lax.broadcasted_iota(jnp.int32, (256, 128), 0).astype(jnp.float32)
    sums = jnp.zeros((256, 512), jnp.float32)
    for a in range(4):
        places, highs, lows = [], [], []
        for b in range(4):
            t = a * 4 + b
            hit = jnp.broadcast_to(marks[t : t + 1, :], (256, 128)) == spots
            places.append(jnp.where(hit, 1.0, 0.0).astype(jnp.bfloat16))
            values = jnp.concatenate(
                [part_ref[pl.ds(pack_row(a, r // 2, b, r % 2), 128, stride=PACK), :] for r in range(4)], axis=1
            )
            high, low = split(values)
            highs.append(high)
            lows.append(low)
        place = jnp.concatenate(places + places, axis=1)
        sums = sums + jnp.dot(place, jnp.concatenate(highs + lows, axis=0), preferred_element_type=jnp.float32)
    for r in range(4):
        out_ref[pl.ds(r, 256, stride=4), :] = sums[:, r * 128 : (r + 1) * 128]


def combine(parts):
    parts = pltpu.with_memory_space_constraint(parts, pltpu.VMEM)
    return pl.pallas_call(
        combine_kernel,
        in_specs=[pl.BlockSpec(memory_space=pltpu.VMEM)],
        out_specs=pl.BlockSpec(memory_space=pltpu.VMEM),
        out_shape=pltpu.VMEM((1024, 128), jnp.float32),
        compiler_params=pltpu.CompilerParams(vmem_limit_bytes=24 * 1024 * 1024),
        name="combine",
    )(parts)


def on_device(inverse_interior, coupling, interface_block, iface_ids, row_place, col_place):
    pieces = schur_tiles(
        iface_ids[0, 0], row_place, col_place, inverse_interior[0, 0], coupling[0, 0], interface_block[0, 0]
    )
    arrived = lax.all_to_all(pieces.reshape(128, PACK, 1, 128), AXES, 0, 0, tiled=True)
    total = combine(arrived.reshape(128 * PACK, 128))
    owned = lax.all_to_all(total.reshape(128, 8, 128), AXES, 0, 0, tiled=True)
    owned = owned.reshape(128, 2, 2, 2, 128).transpose(1, 2, 0, 3, 4)
    return owned.reshape(2, TILE, 1, TILE)


def solution(mesh):
    return jax.shard_map(
        on_device,
        mesh=mesh,
        in_specs=(
            P("row", "col", None, None),
            P("row", "col", None, None),
            P("row", "col", None, None),
            P("row", "col", None),
            P(),
            P(),
        ),
        out_specs=P("row", None, "col", None),
        check_vma=False,
    )
```
